32 devices in a mesh: ba: 8 (over y, x, core), wa: 4 (over z).
Axes of the slice: x: 2, y: 2, z: 4, core: 2. Of those that a mesh axis runs over, the one named last changes fastest.
Arguments:
- sky_model: float32 [2, 2048, 2048], P(None, None, 'wa'), may hold values from -6 to 6
- plane_w: float32 [8], P('ba'), may hold values from -60 to 60
- kernel: float32 [16, 8], replicated, may hold values from -2 to 2
- tile_ids: int32 [512], P(('ba', 'wa')), may hold values from 0 to 255, as said below
- plane_ids: int32 [512, 1], P(('ba', 'wa')), may hold values from 0 to 7; in each aligned block of 16 rows (0 to 15, 16 to 31, ...) at most 2 rows name the same one
- positions: int32 [512, 2, 512], P(('ba', 'wa')), may hold values from 0 to 1935
- observed: float32 [512, 2, 512], P(('ba', 'wa')), may hold values from -6 to 6
Outputs:
- residual_vis: float32 [512, 2, 512], P(('ba', 'wa'))
The draws below stay inside these ranges and needn't reach their ends.
Inputs may be any that keep to these rules, and one draw needn't show every extreme that they name: `plane_ids`: among the 16 blocks of one device at most 2 name the same w-plane, and in every draw some device has a w-plane named by exactly 2 of its blocks. `tile_ids`: A tile id is row_tile * 16 + column_tile; the blocks held at index a of wa name column tiles a * 4 to (a + 1) * 4 - 1.
All inputs are finite; a program needn't handle non-finite values.
Results may differ from the reference program's by a relative error of at most 0.0003.
Values sent between devices are 32-bit elements; how exact they have to be, the bound alone decides.
A program may use at most 128 MiB of HBM per device.

```python
import math
import jax
import jax.numpy as jnp
import numpy as np
from jax import lax

N = 2048
TILE = 128
SUPPORT = 8
OVER = 16
SAMPLES = 512
BLK_DEV = 16
PLANES = 8
CAP = 2
NT = 16
NT_DEV = 4
BLOCKS = 512
N_BA = 8
N_WA = 4


def draw_tile_ids(key, part):
    row_key = jax.random.fold_in(key, 11)
    column_key = jax.random.fold_in(key, 12)
    row_tile = jax.random.randint(row_key, (BLOCKS,), 0, NT, dtype=jnp.int32)
    local_column = jax.random.randint(column_key, (BLOCKS,), 0, NT_DEV, dtype=jnp.int32)
    slab_index = jnp.arange(BLOCKS, dtype=jnp.int32) // BLK_DEV % N_WA
    return row_tile * NT + slab_index * NT_DEV + local_column


def with_ends(array, own_key, least, high):
    longest = array.shape.index(max(array.shape))
    spots = []
    for shift in (0, 1):
        where = [jax.random.randint(jax.random.fold_in(own_key, axis), (), 0, length) for axis, length in enumerate(array.shape)]
        where[longest] = (where[longest] + shift) % array.shape[longest]
        spots.append(tuple(where))
    return array.at[spots[0]].set(least).at[spots[1]].set(high)


def block_scale(stream_key, extent, pieces, low, largest):
    def one(dim, shards_of):
        steps = jax.random.uniform(jax.random.fold_in(jax.random.fold_in(stream_key, 6), dim), (shards_of,), jnp.float32, low / len(pieces), largest / len(pieces))
        return jnp.repeat(jnp.exp(steps), extent[dim] // shards_of).reshape((-1,) + (1,) * (len(extent) - dim - 1))

    level = one(*pieces[0])
    for cut in pieces[1:]:
        level = level * one(*cut)
    return level


def routed_block(own_key, own, number, rows, number_of, top, limit, lean):
    sequence = jax.random.permutation(own_key, number_of)
    heavy_load, ordinary = shares(number_of, rows * top, limit, lean, True), shares(number_of, rows * top, limit, lean, False)
    places = jnp.arange(number_of)

    def named(sizes, turn):
        used = int((sizes > 0).sum())
        fixed = max(1, used // 4)
        shifted = fixed + (places - fixed + turn * (used - fixed)) % max(1, number_of - fixed)
        return jnp.zeros((number_of,), jnp.int32).at[sequence[jnp.where(places < fixed, places, shifted)]].set(jnp.asarray(sizes, jnp.int32))

    sizes = jnp.where(number % 4 == 0, named(heavy_load, number // 4), named(ordinary, number - number // 4 - 1))
    mixed = jax.random.permutation(jax.random.fold_in(own, 3), number_of)
    source_of, taker = mixed[0:number_of // 2 * 2:2], mixed[1:number_of // 2 * 2:2]
    margin = jnp.minimum(sizes[source_of] - 1, limit - sizes[taker]) // 2
    margin = jnp.where((source_of == sequence[0]) | (taker == sequence[0]) | (sizes[taker] == 0), 0, jnp.maximum(margin, 0))
    shifted = jax.random.randint(jax.random.fold_in(own, 4), (number_of // 2,), 0, 1 << 20) % (margin + 1)
    sizes = sizes.at[source_of].add(-shifted).at[taker].add(shifted)
    items = jnp.searchsorted(jnp.cumsum(sizes), jnp.arange(rows * top), side="right").astype(jnp.int32)
    listing = items.reshape(top, rows).T
    listing = listing[jax.random.permutation(jax.random.fold_in(own, 1), rows)]
    turn = jax.random.randint(jax.random.fold_in(own, 2), (rows, 1), 0, top)
    return jnp.take_along_axis(listing, (jnp.arange(top)[None, :] + turn) % top, axis=1)


def shares(count, total, bound, lean, full):
    portions = [(1 << 20) // math.isqrt(rank ** lean) + 1 for rank in range(1, count + 1)]
    largest = bound if full else min(bound, max(-(-total // count), total * portions[0] // sum(portions)))
    least = 1 if total - largest >= count - 1 else 0
    holding, spare = [largest] + [least] * (count - 1), total - largest - least * (count - 1)
    while spare > 0:
        free = [i for i in range(1, count) if holding[i] < largest] or [i for i in range(1, count) if holding[i] < bound]
        pool, remaining = sum([portions[i] for i in free]), spare
        for i in free:
            extra = min(bound - holding[i], max(1, remaining * portions[i] // pool), spare)
            holding[i] = holding[i] + extra
            spare = spare - extra
    return np.array(holding)


def bell_draw(own_key, extent, spread, limit, split=(), held_as=jnp.bfloat16):
    factor_of = block_scale(own_key, extent, split, -0.22, 0.18) if split else 1.0
    values = jax.random.normal(own_key, extent, jnp.float32) * spread * factor_of
    return jnp.minimum(jnp.maximum(values, -limit), limit).astype(held_as)


def setup_inputs(seed: int = 0) -> dict:
    seeds = jax.random.split(jax.random.key(seed), 8)
    sky_model = bell_draw(seeds[0], (2, N, N), 1.0, 6.0, ((2, 4),), jnp.float32)
    plane_w = jnp.clip(jax.random.uniform(seeds[1], (PLANES,), jnp.float32, -60.0, 60.0) * block_scale(seeds[1], (PLANES,), ((0, 8),), -0.4, 0.0), -60.0, 60.0)
    kernel = bell_draw(seeds[2], (OVER, SUPPORT), 0.35, 2.0, (), jnp.float32)
    tile_ids = draw_tile_ids(jax.random.fold_in(seeds[7], 71), 0)
    plane_ids_keys = jax.random.split(jax.random.fold_in(seeds[4], 1), BLOCKS // BLK_DEV)
    plane_ids_turns = jax.random.permutation(jax.random.fold_in(seeds[4], 3), BLOCKS // BLK_DEV)
    plane_ids = jax.vmap(lambda own, number: routed_block(jax.random.fold_in(seeds[4], 2), own, number, BLK_DEV, PLANES, 1, CAP, 2))(plane_ids_keys, plane_ids_turns).reshape((BLOCKS, 1))
    positions = with_ends(jax.random.randint(seeds[5], (BLOCKS, 2, SAMPLES), 0, (TILE - SUPPORT + 1) * OVER), jax.random.fold_in(seeds[5], 1), 0, ((TILE - SUPPORT + 1) * OVER) - 1).astype(jnp.int32)
    observed = bell_draw(seeds[6], (BLOCKS, 2, SAMPLES), 1.0, 6.0, ((0, 32),), jnp.float32)
    return {"sky_model": sky_model, "plane_w": plane_w, "kernel": kernel, "tile_ids": tile_ids, "plane_ids": plane_ids, "positions": positions, "observed": observed}


FIELD_WIDTH = 0.7

def degrid_blocks(uv_grid, tile_list, fine_position, kernel):
    tiles_across = N // TILE
    row_tile = tile_list // tiles_across
    col_tile = tile_list % tiles_across
    cell_index = fine_position // OVER
    offset_index = fine_position % OVER
    kernel_taps = kernel[offset_index]
    tap_offsets = jnp.arange(SUPPORT, dtype=jnp.int32)
    row_cells = (row_tile * TILE)[:, None, None] + cell_index[:, 0, :, None] + tap_offsets
    col_cells = (col_tile * TILE)[:, None, None] + cell_index[:, 1, :, None] + tap_offsets
    patches = uv_grid[:, row_cells[:, :, :, None], col_cells[:, :, None, :]]
    return jnp.einsum('cmsij,msi,msj->mcs', patches, kernel_taps[:, 0], kernel_taps[:, 1])

def reference(sky_model, plane_w, kernel, tile_ids, plane_ids, positions, observed):
    coordinate = (jnp.arange(N, dtype=jnp.int32).astype(jnp.float32) - N / 2) * (FIELD_WIDTH / N)
    radius_sq = coordinate[:, None] ** 2 + coordinate[None, :] ** 2
    lowered = -radius_sq / (1.0 + jnp.sqrt(1.0 - radius_sq))
    target = plane_ids[:, 0]
    window = N_BA * N_WA * CAP
    sorted_blocks = jnp.argsort(target, stable=True).astype(jnp.int32)
    counts = lax.optimization_barrier(jnp.sum((target[None, :] == jnp.arange(PLANES, dtype=jnp.int32)[:, None]).astype(jnp.int32), axis=1))
    starts = (jnp.cumsum(counts) - counts).astype(jnp.int32)
    padded_order = jnp.concatenate([sorted_blocks, jnp.zeros((window,), jnp.int32)])

    def one_plane(predicted, plane_index):
        phase_angle = -2.0 * math.pi * plane_w[plane_index] * lowered
        cosine = jnp.cos(phase_angle)
        sine_part = jnp.sin(phase_angle)
        plane_image = lax.complex(sky_model[0] * cosine - sky_model[1] * sine_part, sky_model[0] * sine_part + sky_model[1] * cosine)
        spectrum = jnp.fft.fft2(plane_image).T / N
        uv_grid = jnp.stack([jnp.real(spectrum), jnp.imag(spectrum)])
        chosen = lax.dynamic_slice(padded_order, (starts[plane_index],), (window,))
        live_rows = jnp.arange(window, dtype=jnp.int32) < counts[plane_index]
        values_out = degrid_blocks(uv_grid, tile_ids[chosen], positions[chosen], kernel)
        predicted = predicted.at[chosen].add(jnp.where(live_rows[:, None, None], values_out, 0.0))
        return (predicted, None)
    predicted = lax.scan(one_plane, jnp.zeros(observed.shape, jnp.float32), jnp.arange(PLANES, dtype=jnp.int32))[0]
    return observed - predicted
```

```python
import functools
import math

import jax
import jax.numpy as jnp
import numpy as np
from jax import lax
from jax.experimental import pallas as pl
from jax.experimental.pallas import tpu as pltpu
from jax.sharding import PartitionSpec as P

TILE = 128
FIELD_WIDTH = 0.7


def halves(values):
    head = values.astype(jnp.bfloat16)
    rest = (values - head.astype(jnp.float32)).astype(jnp.bfloat16)
    return head, rest


def host_halves(values):
    values = values.astype(np.float32)
    head = values.astype(jnp.bfloat16)
    rest = (values - head.astype(np.float32)).astype(jnp.bfloat16)
    return head, rest


def roots(index, modulus):
    angle = -2.0 * np.pi * (index % modulus) / modulus
    return np.cos(angle), np.sin(angle)


def y_tables(extent):
    panels = extent // TILE
    residue = np.arange(panels, dtype=np.int64)[:, None, None]
    step = np.arange(TILE, dtype=np.int64)[None, :, None]
    row = np.arange(TILE, dtype=np.int64)[None, None, :]
    real, imag = roots((panels * step + residue) * row, extent)
    table = np.concatenate(
        [np.concatenate([real, -imag], axis=2), np.concatenate([imag, real], axis=2)], axis=1
    )
    return host_halves(table)


def x_tables(extent, columns):
    tiles = np.arange(extent // TILE, dtype=np.int64)[:, None, None]
    column = np.arange(columns, dtype=np.int64)[None, :, None]
    cell = np.arange(TILE, dtype=np.int64)[None, None, :]
    real, imag = roots((tiles * TILE + cell) * column, extent)
    return host_halves(np.concatenate([real, imag], axis=2))


def fit(function, top, terms):
    nodes = (np.cos((np.arange(400) + 0.5) * np.pi / 400) + 1.0) * 0.5 * top
    series = np.polynomial.chebyshev.Chebyshev.fit(nodes, function(nodes), terms - 1, domain=[0, top])
    return [float(c) for c in series.convert(kind=np.polynomial.Polynomial).coef]


def horner(coefficients, argument):
    total = coefficients[-1]
    for coefficient in coefficients[-2::-1]:
        total = total * argument + coefficient
    return total


def small_dft(values):
    count = len(values)
    if count == 1:
        return values
    even = small_dft(values[0::2])
    odd = small_dft(values[1::2])
    low, high = [], []
    for k in range(count // 2):
        real, imag = odd[k]
        if k == 0:
            pass
        elif 4 * k == count:
            real, imag = imag, -real
        elif 8 * k == count:
            h = math.sqrt(0.5)
            real, imag = (real + imag) * h, (imag - real) * h
        elif 8 * k == 3 * count:
            h = math.sqrt(0.5)
            real, imag = (imag - real) * h, (real + imag) * -h
        else:
            c = math.cos(-2.0 * math.pi * k / count)
            s = math.sin(-2.0 * math.pi * k / count)
            real, imag = real * c - imag * s, real * s + imag * c
        low.append((even[k][0] + real, even[k][1] + imag))
        high.append((even[k][0] - real, even[k][1] - imag))
    return low + high


def y_kernel(extent, columns, w_ref, sky_ref, head_ref, rest_ref, out_head, out_rest, work):
    panels = extent // TILE
    lanes = sky_ref.shape[2]
    spacing = FIELD_WIDTH / extent
    first = lax.axis_index("wa") * columns + pl.program_id(0) * lanes
    w = w_ref[0]
    edge = 2.0 * (FIELD_WIDTH / 2) ** 2
    lower = fit(lambda r: 1.0 / (1.0 + np.sqrt(1.0 - r)), edge, 7)
    sine = fit(lambda z: np.sin(2 * np.pi * np.sqrt(z)) / np.sqrt(z), 0.25, 7)
    cosine = fit(lambda z: np.cos(2 * np.pi * np.sqrt(z)), 0.25, 7)

    for lane in range(0, lanes, 128):
        x = lax.broadcasted_iota(jnp.int32, (8, 128), 1) + (first + lane)
        x = (x.astype(jnp.float32) - extent / 2) * spacing
        x_sq = x * x

        @pl.loop(0, TILE // 8)
        def _(group):
            base = pl.multiple_of(group * 8, 8)
            values = []
            for panel in range(panels):
                row = lax.broadcasted_iota(jnp.int32, (8, 128), 0) + (base + panel * TILE)
                y = (row.astype(jnp.float32) - extent / 2) * spacing
                radius = x_sq + y * y
                turns = radius * horner(lower, radius) * w
                turns = turns - jnp.round(turns)
                square = turns * turns
                s = turns * horner(sine, square)
                c = horner(cosine, square)
                real = sky_ref[0, pl.ds(base + panel * TILE, 8), pl.ds(lane, 128)]
                imag = sky_ref[1, pl.ds(base + panel * TILE, 8), pl.ds(lane, 128)]
                values.append((real * c - imag * s, real * s + imag * c))
            for residue, (real, imag) in enumerate(small_dft(values)):
                work[residue, pl.ds(base, 8), pl.ds(lane, 128)] = real
                work[residue, pl.ds(base + TILE, 8), pl.ds(lane, 128)] = imag

    def panel_product(residue):
        head, rest = halves(work[residue])
        dot = functools.partial(jnp.dot, preferred_element_type=jnp.float32)
        table = head_ref[residue]
        return dot(table, head) + dot(table, rest) + dot(rest_ref[residue], head)

    per_tile = TILE // panels
    share = 8 // per_tile
    together = 16 // per_tile

    @pl.loop(0, panels // together)
    def _(step):
        products = [panel_product(together * step + i) for i in range(together)]
        for part in range(2):
            rows = slice(part * TILE, (part + 1) * TILE)
            grouped = [product[rows].reshape(TILE // 8, 8, lanes) for product in products]
            at = pl.multiple_of(part * TILE + step * 16, 16)
            for place in range(share):
                cut = slice(place * per_tile, (place + 1) * per_tile)
                head, rest = halves(jnp.concatenate([group[:, cut] for group in grouped], axis=1))
                out_head[:, place, pl.ds(at, 16), :] = head
                out_rest[:, place, pl.ds(at, 16), :] = rest


def tile_kernel(tiles_across, slabs, count, resident, over, tiles_ref, pos_ref, taps_ref, h_head, h_rest, e_head, e_rest, out_ref, rows_head, rows_rest):
    extent = tiles_across * TILE
    samples = pos_ref.shape[2]
    dot = functools.partial(jnp.dot, preferred_element_type=jnp.float32)
    slab = lax.axis_index("wa")
    cell = lax.broadcasted_iota(jnp.int32, (1, TILE), 1)
    angle = ((cell * slab) % slabs).astype(jnp.float32) * (-2.0 * math.pi / slabs)
    turn_real = jnp.cos(angle) * (1.0 / extent)
    turn_imag = jnp.sin(angle) * (1.0 / extent)
    place = lax.broadcasted_iota(jnp.int32, (TILE, 128), 0)
    u_start = place * over + over - 1
    groups = tiles_across
    per = TILE // groups
    v_start = ((place % per) * groups + place // per) * over + over - 1
    table = jnp.broadcast_to(taps_ref[...], (TILE, 128))

    def weights(start, position):
        index = start - position
        inside = (index & -128) == 0
        found = jnp.take_along_axis(table, index & 127, axis=1, mode="promise_in_bounds")
        return jnp.where(inside, found, 0.0)

    def one_block(block, row_tile, col_tile):
        head = h_head[col_tile]
        table_head = e_head[row_tile]
        both = dot(head, table_head) + dot(head, e_rest[row_tile]) + dot(h_rest[col_tile], table_head)
        real = both[:TILE, :TILE] - both[TILE:, TILE:]
        imag = both[:TILE, TILE:] + both[TILE:, :TILE]
        grid = jnp.concatenate(
            [real * turn_real - imag * turn_imag, real * turn_imag + imag * turn_real], axis=0
        )
        grid_head, grid_rest = halves(grid)
        for lane in range(0, samples, 128):
            head, rest = halves(weights(u_start, pos_ref[block, 0:1, pl.ds(lane, 128)]))
            rows_head[:, lane : lane + 128] = head
            rows_rest[:, lane : lane + 128] = rest
        head = rows_head[...]
        part = dot(grid_head, head) + dot(grid_head, rows_rest[...]) + dot(grid_rest, head)
        for lane in range(0, samples, 128):
            column = weights(v_start, pos_ref[block, 1:2, pl.ds(lane, 128)])
            for c in range(2):
                values = part[c * TILE : (c + 1) * TILE, lane : lane + 128] * column
                out_ref[block, c : c + 1, lane : lane + 128] = jnp.sum(values, axis=0, keepdims=True)

    if resident:

        @pl.loop(0, count)
        def _(block):
            tile = tiles_ref[block]
            one_block(block, tile // tiles_across, tile % tiles_across)

    else:
        one_block(0, 0, 0)


def shards(sky_model, plane_w, kernel, tile_ids, plane_ids, positions, observed):
    extent, columns = sky_model.shape[1:]
    planes, slabs = lax.axis_size("ba"), lax.axis_size("wa")
    devices = planes * slabs
    block_count, _, samples = positions.shape
    tiles_across = extent // TILE
    capacity = max(2, block_count // planes)
    slots = planes * capacity

    target = plane_ids[:, 0]
    same = target[:, None] == target[None, :]
    before = np.tril(np.ones((block_count, block_count), bool), -1)
    rank = jnp.sum((same & before).astype(jnp.int32), axis=1)
    slot_index = target * capacity + rank
    chosen = slot_index[:, None] == jnp.arange(slots, dtype=jnp.int32)[None, :]
    record = jnp.concatenate(
        [
            positions.reshape(block_count, 2 * samples),
            jnp.broadcast_to(tile_ids[:, None], (block_count, 128)),
        ],
        axis=1,
    )
    length = record.shape[1]
    asked = jnp.sum(jnp.where(chosen[:, :, None], record[:, None, :], 0), axis=0)
    asked = jnp.broadcast_to(
        asked.reshape(planes, 1, capacity, length), (planes, slabs, capacity, length)
    ).reshape(devices, capacity, length)
    axes = ("ba", "wa")
    asked = lax.all_to_all(asked, axes, split_axis=0, concat_axis=0, tiled=True)
    count = devices * capacity
    asked = asked.reshape(count, length)
    asked_fine = asked[:, : 2 * samples].reshape(count, 2, samples)
    asked_tiles = asked[:, 2 * samples]

    lanes = min(columns, 256)
    share = tiles_across * 8 // TILE
    folded = (tiles_across // share, share)
    y_head, y_rest = y_tables(extent)
    vmem = pl.BlockSpec(memory_space=pltpu.VMEM)
    h_head, h_rest = pl.pallas_call(
        functools.partial(y_kernel, extent, columns),
        grid=(columns // lanes,),
        in_specs=[
            pl.BlockSpec(memory_space=pltpu.SMEM),
            pl.BlockSpec((2, extent, lanes), lambda i: (0, 0, i)),
            pl.BlockSpec(y_head.shape, lambda i: (0, 0, 0), pipeline_mode=pl.Buffered(1)),
            pl.BlockSpec(y_rest.shape, lambda i: (0, 0, 0), pipeline_mode=pl.Buffered(1)),
        ],
        out_specs=[pl.BlockSpec(folded + (2 * TILE, lanes), lambda i: (0, 0, 0, i))] * 2,
        out_shape=[jax.ShapeDtypeStruct(folded + (2 * TILE, columns), jnp.bfloat16)] * 2,
        scratch_shapes=[pltpu.VMEM((tiles_across, 2 * TILE, lanes), jnp.float32)],
        compiler_params=pltpu.CompilerParams(vmem_limit_bytes=60 << 20),
        cost_estimate=pl.CostEstimate(
            flops=24 * extent * TILE * columns, bytes_accessed=32 * extent * columns, transcendentals=0
        ),
        name="y_transform",
    )(plane_w, sky_model, jnp.asarray(y_head), jnp.asarray(y_rest))
    h_head = h_head.reshape(tiles_across, 2 * TILE, columns)
    h_rest = h_rest.reshape(tiles_across, 2 * TILE, columns)

    over, support = kernel.shape
    taps = kernel[::-1, :].T.reshape(1, over * support)
    e_head, e_rest = x_tables(extent, columns)
    resident = 4 * tiles_across * 4 * TILE * columns * 2 <= 40 << 20
    if resident:
        layout = {
            "in_specs": [pl.BlockSpec(memory_space=pltpu.SMEM)] + [vmem] * 6,
            "out_specs": vmem,
            "scratch_shapes": [pltpu.VMEM((TILE, samples), jnp.bfloat16)] * 2,
        }
    else:
        own = pl.BlockSpec((1, 2, samples), lambda i, t: (i, 0, 0))
        side = pl.BlockSpec((1, 2 * TILE, columns), lambda i, t: (t[i] % tiles_across, 0, 0))
        table = pl.BlockSpec((1, columns, 2 * TILE), lambda i, t: (t[i] // tiles_across, 0, 0))
        layout = {
            "grid_spec": pltpu.PrefetchScalarGridSpec(
                num_scalar_prefetch=1,
                grid=(count,),
                in_specs=[own, vmem, side, side, table, table],
                out_specs=own,
                scratch_shapes=[pltpu.VMEM((TILE, samples), jnp.bfloat16)] * 2,
            )
        }
    values = pl.pallas_call(
        functools.partial(tile_kernel, tiles_across, slabs, count, resident, over),
        **layout,
        out_shape=jax.ShapeDtypeStruct((count, 2, samples), jnp.float32),
        compiler_params=pltpu.CompilerParams(vmem_limit_bytes=60 << 20),
        cost_estimate=pl.CostEstimate(
            flops=count * 12 * TILE * TILE * (columns + samples), bytes_accessed=32 << 20, transcendentals=0
        ),
        name="tile_degrid",
    )(asked_tiles, asked_fine, taps, h_head, h_rest, jnp.asarray(e_head), jnp.asarray(e_rest))

    values = values.reshape(devices, capacity, 2 * samples)
    answers = lax.all_to_all(values, axes, split_axis=0, concat_axis=0, tiled=True)
    answers = jnp.sum(answers.reshape(planes, slabs, capacity, 2 * samples), axis=1)
    answers = answers.reshape(slots, 2 * samples)
    predicted = jnp.sum(jnp.where(chosen[:, :, None], answers[None], 0.0), axis=1)
    return observed - predicted.reshape(observed.shape)


def solution(mesh):
    return jax.shard_map(
        shards,
        mesh=mesh,
        in_specs=(
            P(None, None, "wa"),
            P("ba"),
            P(),
            P(("ba", "wa")),
            P(("ba", "wa"), None),
            P(("ba", "wa"), None, None),
            P(("ba", "wa"), None, None),
        ),
        out_specs=P(("ba", "wa"), None, None),
        check_vma=False,
    )
```

```python
import functools
import math

import jax
import jax.numpy as jnp
import numpy as np
from jax import lax
from jax.experimental import pallas as pl
from jax.experimental.pallas import tpu as pltpu
from jax.sharding import PartitionSpec as P

TILE = 128
FIELD_WIDTH = 0.7


def halves(values):
    head = values.astype(jnp.bfloat16)
    rest = (values - head.astype(jnp.float32)).astype(jnp.bfloat16)
    return head, rest


def host_halves(values):
    values = values.astype(np.float32)
    head = values.astype(jnp.bfloat16)
    rest = (values - head.astype(np.float32)).astype(jnp.bfloat16)
    return head, rest


def roots(index, modulus):
    angle = -2.0 * np.pi * (index % modulus) / modulus
    return np.cos(angle), np.sin(angle)


def y_tables(extent):
    panels = extent // TILE
    residue = np.arange(panels, dtype=np.int64)[:, None, None]
    step = np.arange(TILE, dtype=np.int64)[None, :, None]
    row = np.arange(TILE, dtype=np.int64)[None, None, :]
    real, imag = roots((panels * step + residue) * row, extent)
    table = np.concatenate(
        [np.concatenate([real, -imag], axis=2), np.concatenate([imag, real], axis=2)], axis=1
    )
    return host_halves(table)


def x_tables(extent, columns):
    tiles = np.arange(extent // TILE, dtype=np.int64)[:, None, None]
    column = np.arange(columns, dtype=np.int64)[None, :, None]
    cell = np.arange(TILE, dtype=np.int64)[None, None, :]
    real, imag = roots((tiles * TILE + cell) * column, extent)
    return host_halves(np.concatenate([real, imag], axis=2))


def fit(function, top, terms):
    nodes = (np.cos((np.arange(400) + 0.5) * np.pi / 400) + 1.0) * 0.5 * top
    series = np.polynomial.chebyshev.Chebyshev.fit(nodes, function(nodes), terms - 1, domain=[0, top])
    return [float(c) for c in series.convert(kind=np.polynomial.Polynomial).coef]


def horner(coefficients, argument):
    total = coefficients[-1]
    for coefficient in coefficients[-2::-1]:
        total = total * argument + coefficient
    return total


def small_dft(values):
    count = len(values)
    if count == 1:
        return values
    even = small_dft(values[0::2])
    odd = small_dft(values[1::2])
    low, high = [], []
    for k in range(count // 2):
        real, imag = odd[k]
        if k == 0:
            pass
        elif 4 * k == count:
            real, imag = imag, -real
        elif 8 * k == count:
            h = math.sqrt(0.5)
            real, imag = (real + imag) * h, (imag - real) * h
        elif 8 * k == 3 * count:
            h = math.sqrt(0.5)
            real, imag = (imag - real) * h, (real + imag) * -h
        else:
            c = math.cos(-2.0 * math.pi * k / count)
            s = math.sin(-2.0 * math.pi * k / count)
            real, imag = real * c - imag * s, real * s + imag * c
        low.append((even[k][0] + real, even[k][1] + imag))
        high.append((even[k][0] - real, even[k][1] - imag))
    return low + high


def lane_lookup(table, index):
    numbers = lax.GatherDimensionNumbers(
        offset_dims=(),
        collapsed_slice_dims=(1,),
        start_index_map=(1,),
        operand_batching_dims=(0,),
        start_indices_batching_dims=(0,),
    )
    return lax.gather(
        table, index[..., None], numbers, (1, 1), mode=lax.GatherScatterMode.PROMISE_IN_BOUNDS
    )


def dot_exact(head_a, rest_a, head_b, rest_b):
    return jnp.dot(
        jnp.concatenate([head_a, head_a, rest_a], axis=1),
        jnp.concatenate([head_b, rest_b, head_b], axis=0),
        preferred_element_type=jnp.float32,
    )


def y_transform(extent, first, w, sky_ref, work):
    panels = extent // TILE
    lanes = sky_ref.shape[2]
    spacing = FIELD_WIDTH / extent
    edge = 2.0 * (FIELD_WIDTH / 2) ** 2
    lower = fit(lambda r: 1.0 / (1.0 + np.sqrt(1.0 - r)), edge, 7)
    sine = fit(lambda z: np.sin(2 * np.pi * np.sqrt(z)) / np.sqrt(z), 0.25, 7)
    cosine = fit(lambda z: np.cos(2 * np.pi * np.sqrt(z)), 0.25, 7)

    for lane in range(0, lanes, 128):
        x = lax.broadcasted_iota(jnp.int32, (8, 128), 1) + (first + lane)
        x = (x.astype(jnp.float32) - extent / 2) * spacing
        x_sq = x * x

        @pl.loop(0, TILE // 8)
        def _(group):
            base = pl.multiple_of(group * 8, 8)
            values = []
            for panel in range(panels):
                row = lax.broadcasted_iota(jnp.int32, (8, 128), 0) + (base + panel * TILE)
                y = (row.astype(jnp.float32) - extent / 2) * spacing
                radius = x_sq + y * y
                turns = radius * horner(lower, radius) * w
                turns = turns - jnp.round(turns)
                square = turns * turns
                s = turns * horner(sine, square)
                c = horner(cosine, square)
                real = sky_ref[0, pl.ds(base + panel * TILE, 8), pl.ds(lane, 128)]
                imag = sky_ref[1, pl.ds(base + panel * TILE, 8), pl.ds(lane, 128)]
                values.append((real * c - imag * s, real * s + imag * c))
            for residue, (real, imag) in enumerate(small_dft(values)):
                work[residue, pl.ds(base, 8), pl.ds(lane, 128)] = real
                work[residue, pl.ds(base + TILE, 8), pl.ds(lane, 128)] = imag


def y_finish(extent, start, work, table_head, table_rest, h_head, h_rest):
    panels = extent // TILE
    lanes = work.shape[2]
    per_tile = TILE // panels
    share = 8 // per_tile
    together = 16 // per_tile

    @pl.loop(0, panels // together)
    def _(step):
        products = []
        for i in range(together):
            residue = together * step + i
            head, rest = halves(work[residue])
            products.append(dot_exact(table_head[residue], table_rest[residue], head, rest))
        for part in range(2):
            rows = slice(part * TILE, (part + 1) * TILE)
            grouped = [product[rows].reshape(TILE // 8, 8, lanes) for product in products]
            at = pl.multiple_of(part * TILE + step * 16, 16)
            for place in range(share):
                cut = slice(place * per_tile, (place + 1) * per_tile)
                head, rest = halves(jnp.concatenate([group[:, cut] for group in grouped], axis=1))
                h_head[:, place, pl.ds(at, 16), pl.ds(start, lanes)] = head
                h_rest[:, place, pl.ds(at, 16), pl.ds(start, lanes)] = rest


def plane_kernel(
    extent, slabs, over, unroll,
    tiles_ref, w_ref, sky_ref, asked_ref, taps_ref, y_head, y_rest, e_head, e_rest, out_ref,
    work, h_head, h_rest, yh, yr, eh, er, rows_head, rows_rest, sems,
):
    tiles_across = extent // TILE
    columns = eh.shape[1]
    lanes = sky_ref.shape[2]
    chunk = pl.program_id(0)
    slab = lax.axis_index("wa")
    share = h_head.shape[1]
    copies = [
        pltpu.make_async_copy(source, target, sems.at[i])
        for i, (source, target) in enumerate(((y_head, yh), (y_rest, yr), (e_head, eh), (e_rest, er)))
    ]

    @pl.when(chunk == 0)
    def _():
        for copy in copies:
            copy.start()

    y_transform(extent, slab * columns + chunk * lanes, w_ref[0], sky_ref, work)

    @pl.when(chunk == 0)
    def _():
        copies[0].wait()
        copies[1].wait()

    y_finish(extent, pl.multiple_of(chunk * lanes, lanes), work, yh, yr, h_head, h_rest)

    @pl.when(chunk == columns // lanes - 1)
    def _():
        copies[2].wait()
        copies[3].wait()
        owners, capacity, length = out_ref.shape
        samples = length // 2
        cell = lax.broadcasted_iota(jnp.int32, (1, TILE), 1)
        angle = ((cell * slab) % slabs).astype(jnp.float32) * (-2.0 * math.pi / slabs)
        turn_real = jnp.cos(angle) * (1.0 / extent)
        turn_imag = jnp.sin(angle) * (1.0 / extent)
        per = TILE // tiles_across

        def weights(axis, position):
            place = lax.broadcasted_iota(jnp.int32, (TILE, 128), 0)
            if axis == 1:
                place = (place % per) * tiles_across + place // per
            index = place * over + (over - 1) - position
            table = jnp.broadcast_to(taps_ref[...], (TILE, 128))
            return jnp.where((index & -128) == 0, lane_lookup(table, index & 127), 0.0)

        def form_tile(tile):
            row_tile = tile // tiles_across
            col_tile = tile % tiles_across
            group, place = col_tile // share, col_tile % share
            both = dot_exact(h_head[group, place], h_rest[group, place], eh[row_tile], er[row_tile])
            real = both[:TILE, :TILE] - both[TILE:, TILE:]
            imag = both[:TILE, TILE:] + both[TILE:, :TILE]
            return halves(
                jnp.concatenate(
                    [real * turn_real - imag * turn_imag, real * turn_imag + imag * turn_real], axis=0
                )
            )

        def row_weights(spot, owner, place):
            for lane in range(0, samples, 128):
                head, rest = halves(weights(0, asked_ref[owner, place : place + 1, lane : lane + 128]))
                rows_head[spot, :, lane : lane + 128] = head
                rows_rest[spot, :, lane : lane + 128] = rest

        def predict(spot, owner, place, tile_pair):
            part = dot_exact(*tile_pair, rows_head[spot], rows_rest[spot])
            for lane in range(0, samples, 128):
                at = samples + lane
                column = weights(1, asked_ref[owner, place : place + 1, at : at + 128])
                for c in range(2):
                    values = part[c * TILE : (c + 1) * TILE, lane : lane + 128] * column
                    at = c * samples + lane
                    out_ref[owner, place : place + 1, at : at + 128] = jnp.sum(
                        values, axis=0, keepdims=True
                    )

        @pl.loop(0, owners // unroll)
        def _(step):
            work_list = [(step * unroll + o, c) for o in range(unroll) for c in range(capacity)]
            tiles = [tiles_ref[owner * capacity + c] for owner, c in work_list]
            pairs = {}
            for spot, (owner, c) in enumerate(work_list):
                row_weights(spot, owner, c)
                pairs[spot] = form_tile(tiles[spot])
                if spot:
                    predict(spot - 1, *work_list[spot - 1], pairs.pop(spot - 1))
            predict(spot, *work_list[spot], pairs.pop(spot))


def pack_kernel(planes_ref, tiles_ref, pos_ref, out_ref, used):
    planes, slabs, capacity, length = out_ref.shape
    blocks, _, samples = pos_ref.shape
    for p in range(planes):
        used[p] = 0

    @pl.loop(0, planes)
    def _(p):
        for a in range(slabs):
            out_ref[p, a] = jnp.zeros((capacity, length), jnp.int32)

    @pl.loop(0, blocks)
    def _(b):
        p = planes_ref[b]
        k = used[p]
        used[p] = k + 1
        for place in range(capacity):

            @pl.when(k == place)
            def _():
                for a in range(slabs):
                    for axis in range(2):
                        cut = slice(axis * samples, (axis + 1) * samples)
                        out_ref[p, a, place : place + 1, cut] = pos_ref[b, axis : axis + 1, :]
                    out_ref[p, a, place : place + 1, 2 * samples :] = jnp.full(
                        (1, 128), tiles_ref[b], jnp.int32
                    )


def residual_kernel(planes, slabs, planes_ref, answers_ref, observed_ref, out_ref, used):
    blocks, _, samples = observed_ref.shape
    for p in range(planes):
        used[p] = 0

    @pl.loop(0, blocks)
    def _(b):
        p = planes_ref[b]
        k = used[p]
        used[p] = k + 1
        total = answers_ref[p * slabs]
        for a in range(1, slabs):
            total += answers_ref[p * slabs + a]
        own = total[0:1]
        for place in range(1, total.shape[0]):
            own = jnp.where(k == place, total[place : place + 1], own)
        for c in range(2):
            out_ref[b, c : c + 1, :] = (
                observed_ref[b, c : c + 1, :] - own[:, c * samples : (c + 1) * samples]
            )


def shards(sky_model, plane_w, kernel, tile_ids, plane_ids, positions, observed):
    extent, columns = sky_model.shape[1:]
    planes, slabs = lax.axis_size("ba"), lax.axis_size("wa")
    devices = planes * slabs
    block_count, _, samples = positions.shape
    tiles_across = extent // TILE
    capacity = max(2, block_count // planes)
    target = plane_ids[:, 0]
    axes = ("ba", "wa")
    smem = pl.BlockSpec(memory_space=pltpu.SMEM)
    vmem = pl.BlockSpec(memory_space=pltpu.VMEM)
    hbm = pl.BlockSpec(memory_space=pl.ANY)
    length = 2 * samples + 128

    asked = pl.pallas_call(
        pack_kernel,
        in_specs=[smem, smem, vmem],
        out_specs=vmem,
        out_shape=jax.ShapeDtypeStruct((planes, slabs, capacity, length), jnp.int32),
        scratch_shapes=[pltpu.SMEM((planes,), jnp.int32)],
        name="pack",
    )(target, tile_ids, positions)
    asked = asked.reshape(devices, capacity, length)
    asked = lax.all_to_all(asked, axes, split_axis=0, concat_axis=0, tiled=True)
    asked_tiles = asked[:, :, 2 * samples].reshape(devices * capacity)

    lanes = min(columns, 256)
    share = tiles_across * 8 // TILE
    unroll = 2
    over, support = kernel.shape
    taps = kernel[::-1, :].T.reshape(1, over * support)
    y_head, y_rest = y_tables(extent)
    e_head, e_rest = x_tables(extent, columns)
    once = pl.Buffered(1)
    answer_shape = (devices, capacity, 2 * samples)
    half = jnp.bfloat16
    values = pl.pallas_call(
        functools.partial(plane_kernel, extent, slabs, over, unroll),
        grid=(columns // lanes,),
        in_specs=[
            smem,
            smem,
            pl.BlockSpec((2, extent, lanes), lambda i: (0, 0, i)),
            pl.BlockSpec(asked.shape, lambda i: (0, 0, 0), pipeline_mode=once),
            pl.BlockSpec(taps.shape, lambda i: (0, 0), pipeline_mode=once),
            hbm, hbm, hbm, hbm,
        ],
        out_specs=pl.BlockSpec(answer_shape, lambda i: (0, 0, 0)),
        out_shape=jax.ShapeDtypeStruct(answer_shape, jnp.float32),
        scratch_shapes=[
            pltpu.VMEM((tiles_across, 2 * TILE, lanes), jnp.float32),
            pltpu.VMEM((tiles_across // share, share, 2 * TILE, columns), half),
            pltpu.VMEM((tiles_across // share, share, 2 * TILE, columns), half),
            pltpu.VMEM(y_head.shape, half),
            pltpu.VMEM(y_head.shape, half),
            pltpu.VMEM(e_head.shape, half),
            pltpu.VMEM(e_head.shape, half),
            pltpu.VMEM((unroll * capacity, TILE, samples), half),
            pltpu.VMEM((unroll * capacity, TILE, samples), half),
            pltpu.SemaphoreType.DMA((4,)),
        ],
        compiler_params=pltpu.CompilerParams(vmem_limit_bytes=60 << 20),
        name="plane",
    )(
        asked_tiles, plane_w, sky_model, asked, taps,
        jnp.asarray(y_head), jnp.asarray(y_rest), jnp.asarray(e_head), jnp.asarray(e_rest),
    )

    answers = lax.all_to_all(values, axes, split_axis=0, concat_axis=0, tiled=True)
    return pl.pallas_call(
        functools.partial(residual_kernel, planes, slabs),
        in_specs=[smem, vmem, vmem],
        out_specs=vmem,
        out_shape=jax.ShapeDtypeStruct(observed.shape, jnp.float32),
        scratch_shapes=[pltpu.SMEM((planes,), jnp.int32)],
        name="residual",
    )(target, answers, observed)


def solution(mesh):
    return jax.shard_map(
        shards,
        mesh=mesh,
        in_specs=(
            P(None, None, "wa"),
            P("ba"),
            P(),
            P(("ba", "wa")),
            P(("ba", "wa"), None),
            P(("ba", "wa"), None, None),
            P(("ba", "wa"), None, None),
        ),
        out_specs=P(("ba", "wa"), None, None),
        check_vma=False,
    )
```
